32 devices in a mesh: row: 4 (over z), col: 8 (over y, x, core).
Axes of the slice: x: 2, y: 2, z: 4, core: 2. Of those that a mesh axis runs over, the one named last changes fastest.
Arguments:
- features: bfloat16 [32768, 256], P(('row', 'col')), may hold values from -6 to 6
- tile_values: bfloat16 [4, 8, 256, 128, 128], P('row', 'col'), may hold values from -0.09375 to 0.09375
- tile_rows: int32 [4, 8, 256], P('row', 'col'), may hold values from 0 to 63, as said below
- tile_cols: int32 [4, 8, 256], P('row', 'col'), may hold values from 0 to 31, as said below
- tile_count: int32 [4, 8], P('row', 'col'), may hold values from 64 to 256, as said below
- w_first: bfloat16 [256, 256], replicated, may hold values from -0.375 to 0.375
- w_second: bfloat16 [256, 256], replicated, may hold values from -0.375 to 0.375
Outputs:
- output: bfloat16 [32768, 256], P(('row', 'col'))
The draws below stay inside these ranges and needn't reach their ends.
Inputs may be any that keep to these rules, and one draw needn't show every extreme that they name: `tile_rows`: in each block the slots name distinct tiles; the first tile_count slots are ordered by tile column, then tile row; later slots are padding. `tile_cols`: as for tile_rows. `tile_count`: some block uses all 256 slots.
All inputs are finite; a program needn't handle non-finite values.
Results may differ from the reference program's by a relative error of at most 0.024.
Values may be sent and summed in bfloat16 or wider, within the bound.
A program may use at most 192 MiB of HBM per device.

```python
import jax
import jax.numpy as jnp
from jax import lax

F = 256
TILE = 128
NODE_DEV = 1024
TILES = 256
TILE_ROWS = 64
TILE_COLS = 32
NODES = 32768
N_ROW = 4
N_COL = 8


def tile_layout(key):
    device_total = N_ROW * N_COL
    slots_total = TILE_ROWS * TILE_COLS
    layout_key = jax.random.fold_in(key, 4242)
    heaviest = jax.random.randint(jax.random.fold_in(layout_key, 1), (), 0, device_total)
    others = jax.random.randint(jax.random.fold_in(layout_key, 2), (device_total,), TILES // 4, TILES + 1)
    counts = jnp.where(jnp.arange(device_total, dtype=jnp.int32) == heaviest, TILES, others).astype(jnp.int32)

    def one_block(device, filled):
        chosen = jax.random.permutation(jax.random.fold_in(layout_key, 100 + device), slots_total)[:TILES]
        slot_ids = jnp.arange(TILES, dtype=jnp.int32)
        marked = jnp.where(slot_ids < filled, chosen, chosen + slots_total).astype(jnp.int32)
        ordered = jnp.sort(marked)
        flat_index = ordered % slots_total
        return (flat_index % TILE_ROWS, flat_index // TILE_ROWS)
    row_ids, col_ids = jax.vmap(one_block)(jnp.arange(device_total, dtype=jnp.int32), counts)
    return (row_ids.reshape(N_ROW, N_COL, TILES).astype(jnp.int32), col_ids.reshape(N_ROW, N_COL, TILES).astype(jnp.int32), counts.reshape(N_ROW, N_COL))


def draw_tile_rows(key, part):
    return tile_layout(key)[0]


def draw_tile_cols(key, part):
    return tile_layout(key)[1]


def draw_tile_count(key, part):
    return tile_layout(key)[2]


def block_levels(rng, shape, pieces, least, largest):
    def one(axis_at, parts):
        draws = jax.random.uniform(jax.random.fold_in(jax.random.fold_in(rng, 6), axis_at), (parts,), jnp.float32, least / len(pieces), largest / len(pieces))
        return jnp.repeat(jnp.exp(draws), shape[axis_at] // parts).reshape((-1,) + (1,) * (len(shape) - axis_at - 1))

    factor_of = one(*pieces[0])
    for cut in pieces[1:]:
        factor_of = factor_of * one(*cut)
    return factor_of


def centred(own_key, extent, width, most, cuts=(), held_as=jnp.bfloat16):
    drawn = jax.random.normal(own_key, extent, jnp.float32) * width
    if len(cuts) > 0:
        drawn = block_levels(own_key, extent, cuts, -0.22, 0.18) * drawn
    return jnp.clip(drawn, min=-most, max=most).astype(held_as)


def setup_inputs(seed: int = 0) -> dict:
    key_of = jax.random.split(jax.random.key(seed), 8)
    return {
        "features": centred(key_of[0], (NODES, F), 1.0, 6.0, ((0, 32),)),
        "tile_values": centred(key_of[1], (N_ROW, N_COL, TILES, TILE, TILE), (TILES * TILE * TILE // NODE_DEV) ** -0.5, 0.09375, ((0, 4), (1, 8))),
        "tile_rows": draw_tile_rows(jax.random.fold_in(key_of[7], 71), 0),
        "tile_cols": draw_tile_cols(jax.random.fold_in(key_of[7], 71), 0),
        "tile_count": draw_tile_count(jax.random.fold_in(key_of[7], 71), 0),
        "w_first": centred(key_of[5], (F, F), F ** -0.5, 0.375),
        "w_second": centred(key_of[6], (F, F), F ** -0.5, 0.375),
    }


def block_partial(values, row_ids, col_ids, filled, panel_tiles):
    active = (jnp.arange(TILES, dtype=jnp.int32) < filled).astype(jnp.float32)
    inputs = panel_tiles[col_ids].astype(jnp.float32)
    products = jnp.einsum("gij,gjf->gif", values.astype(jnp.float32), inputs) * active[:, None, None]
    return jax.ops.segment_sum(products, row_ids, num_segments=TILE_ROWS)


def aggregate(inputs_now, tile_values, tile_rows, tile_cols, tile_count):
    blocks = inputs_now.reshape(N_ROW, N_COL, NODE_DEV, F)

    def row_block(row_index):
        def add_col(running, col_index):
            panel_tiles = blocks[:, col_index].reshape(N_ROW * NODE_DEV // TILE, TILE, F)
            partial_value = block_partial(tile_values[row_index, col_index], tile_rows[row_index, col_index],
                                    tile_cols[row_index, col_index], tile_count[row_index, col_index], panel_tiles)
            rounded = lax.optimization_barrier(partial_value.astype(jnp.bfloat16))
            return running + rounded.astype(jnp.float32), None

        running, unused = lax.scan(add_col, jnp.zeros((TILE_ROWS, TILE, F), jnp.float32),
                                   jnp.arange(N_COL, dtype=jnp.int32))
        return running.astype(jnp.bfloat16)

    summed = lax.map(row_block, jnp.arange(N_ROW, dtype=jnp.int32))
    return summed.reshape(N_ROW * N_COL * NODE_DEV, F)


def reference(features, tile_values, tile_rows, tile_cols, tile_count, w_first, w_second):
    summed = aggregate(features, tile_values, tile_rows, tile_cols, tile_count)
    hidden = jax.nn.relu(jnp.dot(summed, w_first, preferred_element_type=jnp.float32)).astype(jnp.bfloat16)
    summed_two = aggregate(hidden, tile_values, tile_rows, tile_cols, tile_count)
    return jax.nn.relu(jnp.dot(summed_two, w_second, preferred_element_type=jnp.float32)).astype(jnp.bfloat16)
```

```python
import functools

import jax
import jax.numpy as jnp
from jax import lax
from jax.experimental import pallas as pl
from jax.experimental.pallas import tpu as pltpu
from jax.sharding import PartitionSpec as P

LANES = 128
UNROLL_PARTS = 2
LOADS = 4
PARTS = 2
ROWS_AT_ONCE = 256
MESH = pl.DeviceIdType.MESH


def iota(shape, axis):
    return lax.broadcasted_iota(jnp.int32, shape, axis)


def pair_plan(row_ids, col_ids, filled, row_tiles, pairs_total, width):
    slots = row_ids.shape[1]
    one, zero = jnp.int32(1), jnp.int32(0)

    def down(mask):
        return jnp.sum(mask, axis=0, keepdims=True)

    def across(mask):
        return jnp.sum(mask, axis=1, keepdims=True)

    square = (slots, slots)
    lane, sub = iota(square, 1), iota(square, 0)
    rows_l = jnp.where(iota((1, slots), 1) < filled, row_ids, -1)
    rows_s = across(jnp.where(lane == sub, rows_l, zero))
    cols_s = across(jnp.where(lane == sub, col_ids, zero))
    rank_s = across(jnp.where((rows_s == rows_l) & (lane < sub), one, zero))
    hit = jnp.where(rows_s == iota((slots, row_tiles), 1), one, zero)
    hit_t = jnp.where(rows_l == iota((row_tiles, slots), 0), one, zero)
    count_l, count_s = down(hit), across(hit_t)
    pairs_l, pairs_s = (count_l + 1) >> 1, (count_s + 1) >> 1
    box = (row_tiles, row_tiles)
    start_l = down(jnp.where(iota(box, 0) < iota(box, 1), pairs_s, zero))
    start_s = across(jnp.where(iota(box, 1) < iota(box, 0), pairs_l, zero))
    place_s = jnp.where(rows_s >= 0, 2 * across(hit * start_l) + rank_s, -one)
    here = place_s == iota((slots, width), 1)
    slot_ids = iota((slots, width), 0)
    slot_at = slots + down(jnp.where(here, slot_ids - slots, zero))
    col_at = down(jnp.where(here, cols_s, zero))
    opens = (start_s == iota((row_tiles, width), 1)) & (count_s > 0)
    keep = one - down(jnp.where(opens, one, zero))
    last = jnp.where(count_l > 0, start_l + pairs_l - 1, jnp.int32(pairs_total))
    return slot_at, col_at, keep.astype(jnp.float32), last


def kernel(n_row, n_col, chunks, pairs_total, filled, row_ids, col_ids, feat, w1, vals_hbm, out, *scratch):
    phases = 2 * chunks
    panels = scratch[:phases]
    core_in = scratch[phases : 2 * phases]
    step_in = scratch[2 * phases : 3 * phases]
    vals, sums, part, plan_v, keep_v, plan, keep, plan_sem = scratch[3 * phases : 3 * phases + 8]
    load_sem, g_send, g_recv, c_send, c_recv, s_send, s_recv = scratch[3 * phases + 8 :]
    slots, tile, _ = vals_hbm.shape
    node_dev, width = feat.shape
    per_dev = node_dev // tile
    half_tiles = per_dev // 2
    n_q = n_col // 2
    steps = n_q.bit_length() - 1
    block = half_tiles * tile
    half_rows = n_q * block
    r, c = lax.axis_index("row"), lax.axis_index("col")
    b0 = lax.rem(c, 2)
    q = lax.div(c, 2)

    barrier = pltpu.get_barrier_semaphore()
    partners = []
    for bit in range(steps + 1):
        mine = lax.rem(lax.div(c, 1 << bit), 2)
        partners.append((r, c + (1 - 2 * mine) * (1 << bit)))
    for device in partners:
        pl.semaphore_signal(barrier, inc=1, device_id=device, device_id_type=MESH)

    @pl.when(r > 0)
    def _():
        pl.semaphore_signal(barrier, inc=1, device_id=(r - 1, c), device_id_type=MESH)

    @pl.when(r < n_row - 1)
    def _():
        pl.semaphore_signal(barrier, inc=1, device_id=(r + 1, c), device_id_type=MESH)

    share = slots // LOADS
    loads = [
        pltpu.make_async_copy(
            vals_hbm.at[pl.ds(i * share, share)], vals.at[pl.ds(i * share, share)], load_sem.at[i]
        )
        for i in range(LOADS)
    ]
    for load in loads:
        load.start()

    def own(phase, offset, rows):
        return panels[phase].at[pl.ds(r * per_dev + offset, rows)]

    def project(chunk):
        def body(i, carry):
            at = pl.multiple_of(i * ROWS_AT_ONCE, ROWS_AT_ONCE)
            product = jnp.dot(
                feat[pl.ds(at, ROWS_AT_ONCE), :],
                w1[:, chunk * LANES : (chunk + 1) * LANES],
                preferred_element_type=jnp.float32,
            )
            tiles = ROWS_AT_ONCE // tile
            own(chunk, i * tiles, tiles)[...] = product.astype(jnp.bfloat16).reshape(
                tiles, tile, LANES
            )
            return carry

        lax.fori_loop(0, node_dev // ROWS_AT_ONCE, body, 0)

    project(0)
    neighbours = (r > 0).astype(jnp.int32) + (r < n_row - 1).astype(jnp.int32)
    pl.semaphore_wait(barrier, len(partners) + neighbours)

    cut = per_dev // PARTS

    def hop_copy(phase, way, hop, part_id, node, device):
        view = panels[phase].at[pl.ds(node * per_dev + part_id * cut, cut)]
        return pltpu.make_async_remote_copy(
            src_ref=view,
            dst_ref=view,
            send_sem=g_send.at[phase, way, hop - 1, part_id],
            recv_sem=g_recv.at[phase, way, hop - 1, part_id],
            device_id=(device, c),
            device_id_type=MESH,
        )

    def sends(phase, hop, k):
        yield (r < n_row - 1) & (r >= hop - 1), lambda: hop_copy(
            phase, 0, hop, k, r - hop + 1, r + 1
        )
        yield (r > 0) & (r + hop <= n_row), lambda: hop_copy(phase, 1, hop, k, r + hop - 1, r - 1)

    def hop_start(phase, hop, k):
        for cond, make in sends(phase, hop, k):

            @pl.when(cond)
            def _(make=make):
                make().start()

    def hop_wait(phase, hop, k):
        @pl.when(r >= hop)
        def _():
            hop_copy(phase, 0, hop, k, r - hop, r).wait_recv()

        @pl.when(r + hop < n_row)
        def _():
            hop_copy(phase, 1, hop, k, r + hop, r).wait_recv()

    def hop_drain(phase, hop, k):
        for cond, make in sends(phase, hop, k):

            @pl.when(cond)
            def _(make=make):
                make().wait_send()

    class Gather:
        def __init__(self, phase):
            self.phase, self.unit = phase, 0
            self.units = (n_row - 1) * PARTS if phase < phases else 0

        def advance(self, count=1):
            for _ in range(min(count, self.units - self.unit)):
                hop, k = self.unit // PARTS + 1, self.unit % PARTS
                if hop > 1:
                    hop_wait(self.phase, hop - 1, k)
                hop_start(self.phase, hop, k)
                self.unit += 1

        def send_all(self):
            self.advance(self.units)

        def finish(self):
            self.send_all()
            if self.units:
                for k in range(PARTS):
                    hop_wait(self.phase, n_row - 1, k)
                for hop in range(1, n_row):
                    for k in range(PARTS):
                        hop_drain(self.phase, hop, k)

    unroll = pairs_total // UNROLL_PARTS

    def compute(phase, low, high, total):
        panel = panels[phase]

        def one(p, acc):
            left = [vals[plan[0, 2 * p + k]] for k in range(2)]
            right = [panel[plan[1, 2 * p + k]] for k in range(2)]
            product = jnp.dot(
                jnp.concatenate(left, axis=1),
                jnp.concatenate(right, axis=0),
                preferred_element_type=jnp.float32,
            )
            acc = acc * keep[0, p] + product
            sums[p] = acc.astype(jnp.bfloat16)
            return acc

        def body(i, acc):
            for u in range(unroll):
                acc = one(i * unroll + u, acc)
            return acc

        return lax.fori_loop(low // unroll, high // unroll, body, total)

    def place_rows(parity):
        def body(i, carry):
            dq, h = lax.div(i, 2), lax.rem(i, 2)
            dest = 2 * dq + parity
            rev = sum(lax.rem(lax.div(dq, 1 << k), 2) * (1 << (steps - 1 - k)) for k in range(steps))
            at = rev * (1 - h) + dq * h
            base = ((parity * 2 + h) * n_q + at) * half_tiles
            for t in range(half_tiles):
                row_tile = dest * per_dev + h * half_tiles + t
                part[pl.ds(pl.multiple_of((base + t) * tile, tile), tile), :] = sums[
                    plan[2, row_tile]
                ]
            return carry

        lax.fori_loop(0, 2 * n_q, body, 0)

    def add_in(at, source, source_at, rows):
        piece = min(rows, ROWS_AT_ONCE)

        def body(i, carry):
            here = pl.ds(pl.multiple_of(at + i * piece, tile), piece)
            there = pl.ds(pl.multiple_of(source_at + i * piece, tile), piece)
            added = part[here, :].astype(jnp.float32) + source[there, :].astype(jnp.float32)
            part[here, :] = added.astype(jnp.bfloat16)
            return carry

        lax.fori_loop(0, rows // piece, body, 0)

    def remote(src, dst, send_sem, recv_sem, device):
        return pltpu.make_async_remote_copy(
            src_ref=src,
            dst_ref=dst,
            send_sem=send_sem,
            recv_sem=recv_sem,
            device_id=device,
            device_id_type=MESH,
        )

    def rows_at(ref, at, rows):
        return ref.at[pl.ds(pl.multiple_of(at, tile), rows)]

    def mine_at(h, step):
        return lax.rem(lax.div(q, 1 << (step if h == 0 else steps - 1 - step)), 2)

    def pieces(h, step, size):
        if step >= steps:
            return [(0, size)]
        mine = mine_at(h, step)
        return [((1 - mine) * (size // 2), size // 2), (mine * (size // 2), size // 2)]

    def reduce(phase, gather):
        place_rows(1 - b0)
        started = []
        cuts = [pieces(h, 0, half_rows) for h in range(2)]
        arrived = [[], []]
        for k in range(len(cuts[0])):
            for h in range(2):
                off, rows = cuts[h][k]
                copy = remote(
                    rows_at(part, ((1 - b0) * 2 + h) * half_rows + off, rows),
                    rows_at(core_in[phase], h * half_rows + off, rows),
                    c_send.at[phase, h, k],
                    c_recv.at[phase, h, k],
                    partners[0],
                )
                copy.start()
                started.append(copy)
                arrived[h].append((copy, core_in[phase], h * half_rows + off, off, rows))
        gather.advance()
        place_rows(b0)
        gather.advance()
        base = [(b0 * 2 + h) * half_rows for h in range(2)]

        def take(h, k):
            copy, source, source_at, off, rows = arrived[h][k]
            copy.wait_recv()
            add_in(base[h] + off, source, source_at, rows)

        size = half_rows
        for step in range(steps):
            following = [[], []]
            for h in range(2):
                take(h, 0)
                bit = step if h == 0 else steps - 1 - step
                away = base[h] + (1 - mine_at(h, step)) * (size // 2)
                landing = (h * (n_q - 1) + n_q - (n_q >> step)) * block
                for k, (off, rows) in enumerate(pieces(h, step + 1, size // 2)):
                    copy = remote(
                        rows_at(part, away + off, rows),
                        rows_at(step_in[phase], landing + off, rows),
                        s_send.at[phase, h, step, k],
                        s_recv.at[phase, h, step, k],
                        partners[1 + bit],
                    )
                    copy.start()
                    started.append(copy)
                    following[h].append((copy, step_in[phase], landing + off, off, rows))
            for h in range(2):
                take(h, 1)
                base[h] = base[h] + mine_at(h, step) * (size // 2)
            size //= 2
            arrived = following
            gather.advance()
        for h in range(2):
            copy, source, source_at, off, rows = arrived[h][0]
            copy.wait_recv()
            here = pl.ds(pl.multiple_of(base[h], tile), block)
            there = pl.ds(pl.multiple_of(source_at, tile), block)
            added = part[here, :].astype(jnp.float32) + source[there, :].astype(jnp.float32)
            if phase < chunks:
                hidden = jnp.maximum(added, 0.0).astype(jnp.bfloat16)
                own(phase + chunks, h * half_tiles, half_tiles)[...] = hidden.reshape(
                    half_tiles, tile, LANES
                )
            else:
                at = (phase - chunks) * LANES
                out[h * block : (h + 1) * block, at : at + LANES] = added.astype(jnp.bfloat16)
        return started

    vals[slots] = jnp.zeros((tile, tile), vals.dtype)
    sums[pairs_total] = jnp.zeros((tile, LANES), sums.dtype)
    gather = Gather(0)
    gather.advance(PARTS)
    for chunk in range(1, chunks):
        project(chunk)
    slot_at, col_at, keep_at, last = pair_plan(
        row_ids[...], col_ids[...], filled[0, 0], n_col * per_dev, pairs_total, plan.shape[1]
    )
    plan_v[0:1, :] = slot_at
    plan_v[1:2, :] = col_at
    plan_v[2:3, : last.shape[1]] = last
    keep_v[0:1, :] = keep_at
    moves = [
        pltpu.make_async_copy(plan_v, plan, plan_sem.at[0]),
        pltpu.make_async_copy(keep_v, keep, plan_sem.at[1]),
    ]
    gather.advance(PARTS)
    for move in moves:
        move.start()
    for move in moves:
        move.wait()
    for load in loads:
        load.wait()
    following = Gather(1)
    gather.send_all()
    following.advance(PARTS)
    gather.finish()
    for phase in range(phases):
        gather, following = following, Gather(phase + 2)
        middle = UNROLL_PARTS // 2 * unroll
        total = compute(phase, 0, middle, jnp.zeros((tile, LANES), jnp.float32))
        gather.advance()
        compute(phase, middle, UNROLL_PARTS * unroll, total)
        started = reduce(phase, gather)
        gather.send_all()
        following.advance(PARTS)
        for copy in started:
            copy.wait_send()
        gather.finish()


def shards(n_row, n_col, features, tile_values, tile_rows, tile_cols, tile_count, w_first, w_second):
    slots, tile = tile_values.shape[2], tile_values.shape[-1]
    node_dev, width = features.shape
    row_tiles = node_dev * n_col // tile
    chunks = width // LANES
    phases = 2 * chunks
    pairs_total = -(-(slots + row_tiles) // (2 * UNROLL_PARTS)) * UNROLL_PARTS
    n_q = n_col // 2
    steps = n_q.bit_length() - 1
    plan_width = -(-2 * pairs_total // LANES) * LANES
    half = node_dev // 2
    vmem = pl.BlockSpec(memory_space=pltpu.VMEM)
    smem = pl.BlockSpec(memory_space=pltpu.SMEM)
    bf16 = jnp.bfloat16
    dma = pltpu.SemaphoreType.DMA
    aggregate = pl.pallas_call(
        functools.partial(kernel, n_row, n_col, chunks, pairs_total),
        name="gcn",
        out_shape=jax.ShapeDtypeStruct((node_dev, width), bf16),
        in_specs=[smem] + [vmem] * 4 + [pl.BlockSpec(memory_space=pltpu.HBM)],
        out_specs=vmem,
        scratch_shapes=[pltpu.VMEM((n_row * node_dev // tile, tile, LANES), bf16)] * phases
        + [pltpu.VMEM((2 * n_q * half, LANES), bf16)] * phases
        + [pltpu.VMEM((2 * (n_q - 1) * half, LANES), bf16)] * phases
        + [
            pltpu.VMEM((slots + 1, tile, tile), bf16),
            pltpu.VMEM((pairs_total + 1, tile, LANES), bf16),
            pltpu.VMEM((n_col * node_dev, LANES), bf16),
            pltpu.VMEM((8, plan_width), jnp.int32),
            pltpu.VMEM((8, plan_width), jnp.float32),
            pltpu.SMEM((8, plan_width), jnp.int32),
            pltpu.SMEM((8, plan_width), jnp.float32),
            dma((2,)),
            dma((LOADS,)),
            dma((phases, 2, n_row - 1, PARTS)),
            dma((phases, 2, n_row - 1, PARTS)),
            dma((phases, 2, 2)),
            dma((phases, 2, 2)),
            dma((phases, 2, steps, 2)),
            dma((phases, 2, steps, 2)),
        ],
        compiler_params=pltpu.CompilerParams(
            collective_id=0, has_side_effects=True, vmem_limit_bytes=63 * 1024 * 1024
        ),
    )(tile_count, tile_rows[0], tile_cols[0], features, w_first, tile_values[0, 0])
    product = jnp.dot(aggregate, w_second, preferred_element_type=jnp.float32)
    return jax.nn.relu(product).astype(bf16)


def solution(mesh):
    return jax.shard_map(
        functools.partial(shards, mesh.shape["row"], mesh.shape["col"]),
        mesh=mesh,
        in_specs=(
            P(("row", "col"), None),
            P("row", "col", None, None, None),
            P("row", "col", None),
            P("row", "col", None),
            P("row", "col"),
            P(),
            P(),
        ),
        out_specs=P(("row", "col"), None),
        check_vma=False,
    )
```

```python
import functools

import jax
import jax.numpy as jnp
from jax import lax
from jax.experimental import pallas as pl
from jax.experimental.pallas import tpu as pltpu
from jax.sharding import PartitionSpec as P

LANES = 128
UNROLL_PARTS = 2
LOADS = 4
PARTS = 2
ROWS_AT_ONCE = 256
MESH = pl.DeviceIdType.MESH


def iota(shape, axis):
    return lax.broadcasted_iota(jnp.int32, shape, axis)


def pair_plan(row_ids, col_ids, filled, row_tiles, pairs_total, width):
    slots = row_ids.shape[1]
    one, zero = jnp.int32(1), jnp.int32(0)

    def down(mask):
        return jnp.sum(mask, axis=0, keepdims=True)

    def across(mask):
        return jnp.sum(mask, axis=1, keepdims=True)

    square = (slots, slots)
    lane, sub = iota(square, 1), iota(square, 0)
    rows_l = jnp.where(iota((1, slots), 1) < filled, row_ids, -1)
    rows_s = across(jnp.where(lane == sub, rows_l, zero))
    cols_s = across(jnp.where(lane == sub, col_ids, zero))
    rank_s = across(jnp.where((rows_s == rows_l) & (lane < sub), one, zero))
    hit = jnp.where(rows_s == iota((slots, row_tiles), 1), one, zero)
    hit_t = jnp.where(rows_l == iota((row_tiles, slots), 0), one, zero)
    count_l, count_s = down(hit), across(hit_t)
    pairs_l, pairs_s = (count_l + 1) >> 1, (count_s + 1) >> 1
    box = (row_tiles, row_tiles)
    start_l = down(jnp.where(iota(box, 0) < iota(box, 1), pairs_s, zero))
    start_s = across(jnp.where(iota(box, 1) < iota(box, 0), pairs_l, zero))
    place_s = jnp.where(rows_s >= 0, 2 * across(hit * start_l) + rank_s, -one)
    here = place_s == iota((slots, width), 1)
    slot_ids = iota((slots, width), 0)
    slot_at = slots + down(jnp.where(here, slot_ids - slots, zero))
    col_at = down(jnp.where(here, cols_s, zero))
    opens = (start_s == iota((row_tiles, width), 1)) & (count_s > 0)
    keep = one - down(jnp.where(opens, one, zero))
    last = jnp.where(count_l > 0, start_l + pairs_l - 1, jnp.int32(pairs_total))
    return slot_at, col_at, keep.astype(jnp.float32), last


def kernel(n_row, n_col, chunks, pairs_total, filled, row_ids, col_ids, feat_hbm, w1_hbm, vals_hbm, out, *scratch):
    phases = 2 * chunks
    panels = scratch[:phases]
    core_in = scratch[phases : 2 * phases]
    step_in = scratch[2 * phases : 3 * phases]
    feat, w1, vals, sums, part, plan_v, keep_v, plan, keep, plan_sem = scratch[3 * phases : 3 * phases + 10]
    in_sem, load_sem, g_send, g_recv, c_send, c_recv, s_send, s_recv = scratch[3 * phases + 10 :]
    slots, tile, _ = vals_hbm.shape
    node_dev, width = feat.shape
    per_dev = node_dev // tile
    half_tiles = per_dev // 2
    n_q = n_col // 2
    steps = n_q.bit_length() - 1
    block = half_tiles * tile
    half_rows = n_q * block
    r, c = lax.axis_index("row"), lax.axis_index("col")
    b0 = lax.rem(c, 2)
    q = lax.div(c, 2)

    cut = per_dev // PARTS
    cut_rows = cut * tile
    feat_loads = [
        pltpu.make_async_copy(
            feat_hbm.at[pl.ds(k * cut_rows, cut_rows)], feat.at[pl.ds(k * cut_rows, cut_rows)], in_sem.at[k + 1]
        )
        for k in range(PARTS)
    ]
    w1_load = pltpu.make_async_copy(w1_hbm, w1, in_sem.at[0])
    w1_load.start()
    for load in feat_loads:
        load.start()

    barrier = pltpu.get_barrier_semaphore()
    partners = []
    for bit in range(steps + 1):
        mine = lax.rem(lax.div(c, 1 << bit), 2)
        partners.append((r, c + (1 - 2 * mine) * (1 << bit)))
    for device in partners:
        pl.semaphore_signal(barrier, inc=1, device_id=device, device_id_type=MESH)
    greeted = jnp.int32(len(partners))
    last_row = n_row - 1
    distances = [d * sign for d in range(last_row, 0, -1) for sign in (1, -1)]

    def inner(node):
        return (node > 0) & (node < last_row)

    def outer(node):
        return (node == 0) | (node == last_row)

    for d in distances:
        there = r + d
        valid = (there >= 0) & (there <= last_row)
        reached = valid if abs(d) == 1 else valid & inner(there)
        greeted = greeted + reached.astype(jnp.int32)

        @pl.when(valid if abs(d) == 1 else valid & inner(r))
        def _(there=there):
            pl.semaphore_signal(barrier, inc=1, device_id=(there, c), device_id_type=MESH)

    share = slots // LOADS
    loads = [
        pltpu.make_async_copy(
            vals_hbm.at[pl.ds(i * share, share)], vals.at[pl.ds(i * share, share)], load_sem.at[i]
        )
        for i in range(LOADS)
    ]
    for load in loads:
        load.start()

    def own(phase, offset, rows):
        return panels[phase].at[pl.ds(r * per_dev + offset, rows)]

    def project(chunk, k):
        size = min(cut_rows, ROWS_AT_ONCE)
        for at in range(k * cut_rows, (k + 1) * cut_rows, size):
            product = jnp.dot(
                feat[at : at + size, :],
                w1[:, chunk * LANES : (chunk + 1) * LANES],
                preferred_element_type=jnp.float32,
            )
            tiles = size // tile
            own(chunk, at // tile, tiles)[...] = product.astype(jnp.bfloat16).reshape(tiles, tile, LANES)

    def node_copy(phase, origin, d, k, device):
        view = panels[phase].at[pl.ds(origin * per_dev + k * cut, cut)]
        return pltpu.make_async_remote_copy(
            src_ref=view,
            dst_ref=view,
            send_sem=g_send.at[phase, d + n_row - 1, k],
            recv_sem=g_recv.at[phase, d + n_row - 1, k],
            device_id=(device, c),
            device_id_type=MESH,
        )

    def inner_sends(phase, k):
        for d in distances:
            target = r + d
            yield inner(target), node_copy(phase, r, d, k, target)

    def outer_sends(phase, k):
        for d in (1, -1):
            target = r + d
            yield outer(target), node_copy(phase, r, d, k, target)

    def relays(phase, near, k):
        for sign in (1, -1):
            origin = r - sign * near
            place = n_row - 2 if sign > 0 else 1
            valid = (r == place) & (origin >= 0) & (origin <= last_row)
            arrived = node_copy(phase, origin, sign * near, k, r)
            forward = node_copy(phase, origin, sign * (near + 1), k, r + sign)
            yield valid, arrived, forward

    def start_all(sends):
        for valid, copy in sends:
            pl.when(valid)(copy.start)

    def own_inner(phase):
        if phase < phases:
            for k in range(PARTS):
                start_all(inner_sends(phase, k))

    def own_outer(phase):
        if phase < phases:
            for k in range(PARTS):
                start_all(outer_sends(phase, k))

    def relay(phase, near, k):
        if phase < phases:
            for valid, arrived, forward in relays(phase, near, k):

                @pl.when(valid)
                def _(arrived=arrived, forward=forward):
                    arrived.wait_recv()
                    forward.start()

    def relay_far(phase):
        for k in range(PARTS):
            for near in range(2, last_row):
                relay(phase, near, k)

    def relay_all(phase):
        for k in range(PARTS):
            for near in range(1, last_row):
                relay(phase, near, k)

    def gathered(phase):
        for k in range(PARTS):
            for d in sorted(distances, key=abs):
                origin = r - d
                relayed = r == (n_row - 2 if d > 0 else 1)
                valid = (origin >= 0) & (origin <= last_row) & jnp.logical_not(relayed)
                pl.when(valid)(node_copy(phase, origin, d, k, r).wait_recv)

    def drain(phase):
        for k in range(PARTS):
            for valid, copy in [*inner_sends(phase, k), *outer_sends(phase, k)]:
                pl.when(valid)(copy.wait_send)
            for near in range(1, last_row):
                for valid, _, forward in relays(phase, near, k):
                    pl.when(valid)(forward.wait_send)

    unroll = pairs_total // UNROLL_PARTS

    def compute(phase):
        panel = panels[phase]

        def one(p, acc):
            left = [vals[plan[0, 2 * p + k]] for k in range(2)]
            right = [panel[plan[1, 2 * p + k]] for k in range(2)]
            product = jnp.dot(
                jnp.concatenate(left, axis=1),
                jnp.concatenate(right, axis=0),
                preferred_element_type=jnp.float32,
            )
            acc = acc * keep[0, p] + product
            sums[p] = acc.astype(jnp.bfloat16)
            return acc

        def body(i, acc):
            for u in range(unroll):
                acc = one(i * unroll + u, acc)
            return acc

        lax.fori_loop(0, UNROLL_PARTS, body, jnp.zeros((tile, LANES), jnp.float32))

    def place_rows(parity, h, at, count):
        def body(i, carry):
            rev = sum(lax.rem(lax.div(at + i, 1 << k), 2) * (1 << (steps - 1 - k)) for k in range(steps))
            dest = 2 * (rev if h == 0 else at + i) + parity
            base = ((parity * 2 + h) * n_q + at + i) * half_tiles
            for t in range(half_tiles):
                row_tile = dest * per_dev + h * half_tiles + t
                part[pl.ds(pl.multiple_of((base + t) * tile, tile), tile), :] = sums[
                    plan[2, row_tile]
                ]
            return carry

        lax.fori_loop(0, count, body, 0)

    def add_in(at, source, source_at, rows):
        piece = min(rows, ROWS_AT_ONCE)

        def body(i, carry):
            here = pl.ds(pl.multiple_of(at + i * piece, tile), piece)
            there = pl.ds(pl.multiple_of(source_at + i * piece, tile), piece)
            added = part[here, :].astype(jnp.float32) + source[there, :].astype(jnp.float32)
            part[here, :] = added.astype(jnp.bfloat16)
            return carry

        lax.fori_loop(0, rows // piece, body, 0)

    def remote(src, dst, send_sem, recv_sem, device):
        return pltpu.make_async_remote_copy(
            src_ref=src,
            dst_ref=dst,
            send_sem=send_sem,
            recv_sem=recv_sem,
            device_id=device,
            device_id_type=MESH,
        )

    def rows_at(ref, at, rows):
        return ref.at[pl.ds(pl.multiple_of(at, tile), rows)]

    def mine_at(h, step):
        return lax.rem(lax.div(q, 1 << (step if h == 0 else steps - 1 - step)), 2)

    def pieces(h, step, size):
        if step >= steps:
            return [(0, size)]
        mine = mine_at(h, step)
        return [((1 - mine) * (size // 2), size // 2), (mine * (size // 2), size // 2)]

    def reduce(phase):
        started = []
        cuts = [pieces(h, 0, half_rows) for h in range(2)]
        arrived = [[], []]
        for k in range(len(cuts[0])):
            for h in range(2):
                off, rows = cuts[h][k]
                place_rows(1 - b0, h, lax.div(off, block), rows // block)
                copy = remote(
                    rows_at(part, ((1 - b0) * 2 + h) * half_rows + off, rows),
                    rows_at(core_in[phase], h * half_rows + off, rows),
                    c_send.at[phase, h, k],
                    c_recv.at[phase, h, k],
                    partners[0],
                )
                copy.start()
                started.append(copy)
                arrived[h].append((copy, core_in[phase], h * half_rows + off, off, rows))
        for k in range(len(cuts[0])):
            for h in range(2):
                off, rows = cuts[h][k]
                place_rows(b0, h, lax.div(off, block), rows // block)
        base = [(b0 * 2 + h) * half_rows for h in range(2)]

        def take(h, k):
            copy, source, source_at, off, rows = arrived[h][k]
            copy.wait_recv()
            add_in(base[h] + off, source, source_at, rows)

        size = half_rows
        for step in range(steps):
            following = [[], []]
            for h in range(2):
                take(h, 0)
                bit = step if h == 0 else steps - 1 - step
                away = base[h] + (1 - mine_at(h, step)) * (size // 2)
                landing = (h * (n_q - 1) + n_q - (n_q >> step)) * block
                for k, (off, rows) in enumerate(pieces(h, step + 1, size // 2)):
                    copy = remote(
                        rows_at(part, away + off, rows),
                        rows_at(step_in[phase], landing + off, rows),
                        s_send.at[phase, h, step, k],
                        s_recv.at[phase, h, step, k],
                        partners[1 + bit],
                    )
                    copy.start()
                    started.append(copy)
                    following[h].append((copy, step_in[phase], landing + off, off, rows))
            for h in range(2):
                take(h, 1)
                base[h] = base[h] + mine_at(h, step) * (size // 2)
            size //= 2
            arrived = following
            if step == 0:
                for k in range(PARTS):
                    relay(phase + 1, 1, k)
        for h in range(2):
            copy, source, source_at, off, rows = arrived[h][0]
            copy.wait_recv()
            here = pl.ds(pl.multiple_of(base[h], tile), block)
            there = pl.ds(pl.multiple_of(source_at, tile), block)
            added = part[here, :].astype(jnp.float32) + source[there, :].astype(jnp.float32)
            if phase < chunks:
                hidden = jnp.maximum(added, 0.0).astype(jnp.bfloat16)
                own(phase + chunks, h * half_tiles, half_tiles)[...] = hidden.reshape(
                    half_tiles, tile, LANES
                )
            else:
                at = (phase - chunks) * LANES
                out[h * block : (h + 1) * block, at : at + LANES] = added.astype(jnp.bfloat16)
        return started

    w1_load.wait()
    for k in range(PARTS):
        feat_loads[k].wait()
        project(0, k)
        if k == 0:
            pl.semaphore_wait(barrier, greeted)
        start_all(inner_sends(0, k))
        start_all(outer_sends(0, k))
    for chunk in range(1, chunks):
        for k in range(PARTS):
            project(chunk, k)
    pl.when(outer(r))(lambda: own_inner(1))
    vals[slots] = jnp.zeros((tile, tile), vals.dtype)
    sums[pairs_total] = jnp.zeros((tile, LANES), sums.dtype)
    slot_at, col_at, keep_at, last = pair_plan(
        row_ids[...], col_ids[...], filled[0, 0], n_col * per_dev, pairs_total, plan.shape[1]
    )
    plan_v[0:1, :] = slot_at
    plan_v[1:2, :] = col_at
    plan_v[2:3, : last.shape[1]] = last
    keep_v[0:1, :] = keep_at
    moves = [
        pltpu.make_async_copy(plan_v, plan, plan_sem.at[0]),
        pltpu.make_async_copy(keep_v, keep, plan_sem.at[1]),
    ]
    for move in moves:
        move.start()
    relay_all(0)
    for move in moves:
        move.wait()
    for load in loads:
        load.wait()
    pl.when(inner(r))(lambda: own_inner(1))
    own_outer(1)
    for phase in range(phases):
        gathered(phase)
        compute(phase)
        started = reduce(phase)
        if phase < chunks:
            own_inner(phase + chunks)
        if phase + 1 < phases:
            relay_far(phase + 1)
        if phase < chunks:
            own_outer(phase + chunks)
        for copy in started:
            copy.wait_send()
    for phase in range(phases):
        drain(phase)


def shards(n_row, n_col, features, tile_values, tile_rows, tile_cols, tile_count, w_first, w_second):
    slots, tile = tile_values.shape[2], tile_values.shape[-1]
    node_dev, width = features.shape
    row_tiles = node_dev * n_col // tile
    chunks = width // LANES
    phases = 2 * chunks
    pairs_total = -(-(slots + row_tiles) // (2 * UNROLL_PARTS)) * UNROLL_PARTS
    n_q = n_col // 2
    steps = n_q.bit_length() - 1
    plan_width = -(-2 * pairs_total // LANES) * LANES
    half = node_dev // 2
    vmem = pl.BlockSpec(memory_space=pltpu.VMEM)
    smem = pl.BlockSpec(memory_space=pltpu.SMEM)
    bf16 = jnp.bfloat16
    dma = pltpu.SemaphoreType.DMA
    aggregate = pl.pallas_call(
        functools.partial(kernel, n_row, n_col, chunks, pairs_total),
        name="gcn",
        out_shape=pltpu.VMEM((node_dev, width), bf16),
        in_specs=[smem] + [vmem] * 2 + [pl.BlockSpec(memory_space=pltpu.HBM)] * 3,
        out_specs=vmem,
        scratch_shapes=[pltpu.VMEM((n_row * node_dev // tile, tile, LANES), bf16)] * phases
        + [pltpu.VMEM((2 * n_q * half, LANES), bf16)] * phases
        + [pltpu.VMEM((2 * (n_q - 1) * half, LANES), bf16)] * phases
        + [
            pltpu.VMEM((node_dev, width), bf16),
            pltpu.VMEM((width, width), bf16),
            pltpu.VMEM((slots + 1, tile, tile), bf16),
            pltpu.VMEM((pairs_total + 1, tile, LANES), bf16),
            pltpu.VMEM((n_col * node_dev, LANES), bf16),
            pltpu.VMEM((8, plan_width), jnp.int32),
            pltpu.VMEM((8, plan_width), jnp.float32),
            pltpu.SMEM((8, plan_width), jnp.int32),
            pltpu.SMEM((8, plan_width), jnp.float32),
            dma((2,)),
            dma((1 + PARTS,)),
            dma((LOADS,)),
            dma((phases, 2 * n_row - 1, PARTS)),
            dma((phases, 2 * n_row - 1, PARTS)),
            dma((phases, 2, 2)),
            dma((phases, 2, 2)),
            dma((phases, 2, steps, 2)),
            dma((phases, 2, steps, 2)),
        ],
        compiler_params=pltpu.CompilerParams(
            collective_id=0, has_side_effects=True, vmem_limit_bytes=63 * 1024 * 1024
        ),
    )(tile_count, tile_rows[0], tile_cols[0], features, w_first, tile_values[0, 0])
    product = jnp.dot(aggregate, w_second, preferred_element_type=jnp.float32)
    return jax.nn.relu(product).astype(bf16)


def solution(mesh):
    return jax.shard_map(
        functools.partial(shards, mesh.shape["row"], mesh.shape["col"]),
        mesh=mesh,
        in_specs=(
            P(("row", "col"), None),
            P("row", "col", None, None, None),
            P("row", "col", None),
            P("row", "col", None),
            P("row", "col"),
            P(),
            P(),
        ),
        out_specs=P(("row", "col"), None),
        check_vma=False,
    )
```

```python
import functools

import jax
import jax.numpy as jnp
from jax import lax
from jax.experimental import pallas as pl
from jax.experimental.pallas import tpu as pltpu
from jax.sharding import PartitionSpec as P

LANES = 128
UNROLL_PARTS = 2
LOADS = 4
SETS = 3
PARTS = 2
ROWS_AT_ONCE = 256
MESH = pl.DeviceIdType.MESH


def iota(shape, axis):
    return lax.broadcasted_iota(jnp.int32, shape, axis)


def pair_plan(row_ids, col_ids, filled, row_tiles, pairs_total, width):
    slots = row_ids.shape[1]
    one, zero = jnp.int32(1), jnp.int32(0)

    def down(mask):
        return jnp.sum(mask, axis=0, keepdims=True)

    def across(mask):
        return jnp.sum(mask, axis=1, keepdims=True)

    square = (slots, slots)
    lane, sub = iota(square, 1), iota(square, 0)
    rows_l = jnp.where(iota((1, slots), 1) < filled, row_ids, -1)
    rows_s = across(jnp.where(lane == sub, rows_l, zero))
    cols_s = across(jnp.where(lane == sub, col_ids, zero))
    rank_s = across(jnp.where((rows_s == rows_l) & (lane < sub), one, zero))
    hit = jnp.where(rows_s == iota((slots, row_tiles), 1), one, zero)
    hit_t = jnp.where(rows_l == iota((row_tiles, slots), 0), one, zero)
    count_l, count_s = down(hit), across(hit_t)
    pairs_l, pairs_s = (count_l + 1) >> 1, (count_s + 1) >> 1
    box = (row_tiles, row_tiles)
    start_l = down(jnp.where(iota(box, 0) < iota(box, 1), pairs_s, zero))
    start_s = across(jnp.where(iota(box, 1) < iota(box, 0), pairs_l, zero))
    place_s = jnp.where(rows_s >= 0, 2 * across(hit * start_l) + rank_s, -one)
    here = place_s == iota((slots, width), 1)
    slot_ids = iota((slots, width), 0)
    slot_at = slots + down(jnp.where(here, slot_ids - slots, zero))
    col_at = down(jnp.where(here, cols_s, zero))
    opens = (start_s == iota((row_tiles, width), 1)) & (count_s > 0)
    keep = one - down(jnp.where(opens, one, zero))
    last = jnp.where(count_l > 0, start_l + pairs_l - 1, jnp.int32(pairs_total))
    return slot_at, col_at, keep.astype(jnp.float32), last


def kernel(n_row, n_col, chunks, pairs_total, filled, row_ids, col_ids, feat_hbm, w1_hbm, vals_hbm, out, *scratch):
    phases = 2 * chunks + 1
    first, second = phases - 2, phases - 1
    panels = scratch[:phases]
    core_in = scratch[phases : 2 * phases]
    step_in = scratch[2 * phases : 3 * phases]
    feat, w1, vals, sums, wide_part, thin_part, spread, held = scratch[3 * phases : 3 * phases + 8]
    plan_v, keep_v, plan, keep, plan_sem = scratch[3 * phases + 8 : 3 * phases + 13]
    in_sem, load_sem, g_send, g_recv, c_send, c_recv, s_send, s_recv = scratch[3 * phases + 13 :]
    slots, tile, _ = vals_hbm.shape
    node_dev, width = feat.shape
    per_dev = node_dev // tile
    half_tiles = per_dev // 2
    n_q = n_col // 2
    steps = n_q.bit_length() - 1
    low = iota((tile, LANES), 1) < LANES // 2
    r, c = lax.axis_index("row"), lax.axis_index("col")
    b0 = lax.rem(c, 2)
    q = lax.div(c, 2)

    cut = per_dev // PARTS
    cut_rows = cut * tile
    feat_loads = [
        pltpu.make_async_copy(
            feat_hbm.at[pl.ds(k * cut_rows, cut_rows)], feat.at[pl.ds(k * cut_rows, cut_rows)], in_sem.at[k + 1]
        )
        for k in range(PARTS)
    ]
    w1_load = pltpu.make_async_copy(w1_hbm, w1, in_sem.at[0])
    w1_load.start()
    for load in feat_loads:
        load.start()

    barrier = pltpu.get_barrier_semaphore()
    partners = []
    for bit in range(steps + 1):
        mine = lax.rem(lax.div(c, 1 << bit), 2)
        partners.append((r, c + (1 - 2 * mine) * (1 << bit)))
    for device in partners:
        pl.semaphore_signal(barrier, inc=1, device_id=device, device_id_type=MESH)
    greeted = jnp.int32(len(partners))
    last_row = n_row - 1
    distances = [d * sign for d in range(last_row, 0, -1) for sign in (1, -1)]

    def inner(node):
        return (node > 0) & (node < last_row)

    def outer(node):
        return (node == 0) | (node == last_row)

    for d in distances:
        there = r + d
        valid = (there >= 0) & (there <= last_row)
        reached = valid if abs(d) == 1 else valid & inner(there)
        greeted = greeted + reached.astype(jnp.int32)

        @pl.when(valid if abs(d) == 1 else valid & inner(r))
        def _(there=there):
            pl.semaphore_signal(barrier, inc=1, device_id=(there, c), device_id_type=MESH)

    share = slots // LOADS
    loads = [
        pltpu.make_async_copy(
            vals_hbm.at[pl.ds(i * share, share)], vals.at[pl.ds(i * share, share)], load_sem.at[i]
        )
        for i in range(LOADS)
    ]
    for load in loads:
        load.start()

    def node_tiles(phase):
        return per_dev // 2 if phase >= first else per_dev

    def own(phase, offset, rows):
        return panels[phase].at[pl.ds(r * node_tiles(phase) + offset, rows)]

    def turned(value):
        return pltpu.roll(value, LANES // 2, 1)

    def project(chunk, k):
        size = min(cut_rows, ROWS_AT_ONCE)
        for at in range(k * cut_rows, (k + 1) * cut_rows, size):
            product = jnp.dot(
                feat[at : at + size, :],
                w1[:, chunk * LANES : (chunk + 1) * LANES],
                preferred_element_type=jnp.float32,
            )
            tiles = size // tile
            own(chunk, at // tile, tiles)[...] = product.astype(jnp.bfloat16).reshape(tiles, tile, LANES)

    def way(d):
        return d - 1 if d > 0 else last_row - 1 - d

    def node_copy(phase, origin, d, k, device):
        share = node_tiles(phase) // PARTS
        view = panels[phase].at[pl.ds(origin * node_tiles(phase) + k * share, share)]
        return pltpu.make_async_remote_copy(
            src_ref=view,
            dst_ref=view,
            send_sem=g_send.at[phase % SETS, way(d), k],
            recv_sem=g_recv.at[phase, way(d), k],
            device_id=(device, c),
            device_id_type=MESH,
        )

    def inner_sends(phase, k, reaches=range(1, n_row)):
        for d in distances:
            if abs(d) not in reaches:
                continue
            target = r + d
            yield inner(target), node_copy(phase, r, d, k, target)

    def outer_sends(phase, k):
        for d in (1, -1):
            target = r + d
            yield outer(target), node_copy(phase, r, d, k, target)

    def relays(phase, near, k):
        for sign in (1, -1):
            origin = r - sign * near
            place = n_row - 2 if sign > 0 else 1
            valid = (r == place) & (origin >= 0) & (origin <= last_row)
            arrived = node_copy(phase, origin, sign * near, k, r)
            forward = node_copy(phase, origin, sign * (near + 1), k, r + sign)
            yield valid, arrived, forward

    def start_all(sends):
        for valid, copy in sends:
            pl.when(valid)(copy.start)

    def own_inner(phase):
        for reach in range(last_row, 0, -1):
            for k in range(PARTS):
                start_all(inner_sends(phase, k, (reach,)))

    def own_outer(phase):
        if phase < phases:
            for k in range(PARTS):
                start_all(outer_sends(phase, k))

    def relay(phase, near, k):
        if phase < phases:
            for valid, arrived, forward in relays(phase, near, k):

                @pl.when(valid)
                def _(arrived=arrived, forward=forward):
                    arrived.wait_recv()
                    forward.start()

    def relay_far(phase):
        for near in range(2, last_row):
            for k in range(PARTS):
                relay(phase, near, k)

    def relay_near(phase):
        for k in range(PARTS):
            relay(phase, 1, k)

    def relay_all(phase):
        relay_near(phase)
        relay_far(phase)

    def arrive(phase, d, k):
        origin = r - d
        relayed = r == (n_row - 2 if d > 0 else 1)
        valid = (origin >= 0) & (origin <= last_row) & jnp.logical_not(relayed)
        pl.when(valid)(node_copy(phase, origin, d, k, r).wait_recv)

    def gathered(phase):
        for k in range(PARTS):
            for d in sorted(distances, key=abs):
                arrive(phase, d, k)

    def spread_node(phase, origin):
        def body(i, carry):
            at = origin * (per_dev // 2) + i
            pair = panels[phase][at].astype(jnp.float32)
            other = turned(pair)
            spread[2 * at] = jnp.where(low, pair, other).astype(jnp.bfloat16)
            spread[2 * at + 1] = jnp.where(low, other, pair).astype(jnp.bfloat16)
            return carry

        lax.fori_loop(0, per_dev // 2, body, 0, unroll=True)

    def gathered_spread(phase):
        spread_node(phase, r)
        for d in sorted(distances, key=abs):
            for k in range(PARTS):
                arrive(phase, d, k)

            @pl.when((r - d >= 0) & (r - d <= last_row))
            def _(d=d):
                spread_node(phase, r - d)

    def drain(phase):
        for k in range(PARTS):
            for valid, copy in [*inner_sends(phase, k), *outer_sends(phase, k)]:
                pl.when(valid)(copy.wait_send)
            for near in range(1, last_row):
                for valid, _, forward in relays(phase, near, k):
                    pl.when(valid)(forward.wait_send)

    unroll = pairs_total // UNROLL_PARTS

    def compute(panel, low_trip=0, high_trip=UNROLL_PARTS, total=None):
        def one(p, acc):
            left = [vals[plan[0, 2 * p + k]] for k in range(2)]
            right = [panel[plan[1, 2 * p + k]] for k in range(2)]
            product = jnp.dot(
                jnp.concatenate(left, axis=1),
                jnp.concatenate(right, axis=0),
                preferred_element_type=jnp.float32,
            )
            acc = acc * keep[0, p] + product
            sums[p] = acc.astype(jnp.bfloat16)
            return acc

        def body(i, acc):
            for u in range(unroll):
                acc = one(i * unroll + u, acc)
            return acc

        if total is None:
            total = jnp.zeros((tile, LANES), jnp.float32)
        return lax.fori_loop(low_trip, high_trip, body, total)

    def place_rows(part, region, parity, h, at, count, narrow):
        taken = half_tiles // 2 if narrow else half_tiles

        def body(i, carry):
            rev = sum(lax.rem(lax.div(at + i, 1 << k), 2) * (1 << (steps - 1 - k)) for k in range(steps))
            dest = 2 * (rev if h == 0 else at + i) + parity
            base = region + ((parity * 2 + h) * n_q + at + i) * taken
            row_tile = dest * per_dev + h * half_tiles
            for t in range(taken):
                if narrow:
                    rows = jnp.where(
                        low, sums[plan[2, row_tile + 2 * t]], sums[plan[2, row_tile + 2 * t + 1]]
                    )
                else:
                    rows = sums[plan[2, row_tile + t]]
                part[pl.ds(pl.multiple_of((base + t) * tile, tile), tile), :] = rows
            return carry

        lax.fori_loop(0, count, body, 0)

    def add_in(part, at, source, source_at, rows):
        piece = min(rows, ROWS_AT_ONCE)

        def body(i, carry):
            here = pl.ds(pl.multiple_of(at + i * piece, tile), piece)
            there = pl.ds(pl.multiple_of(source_at + i * piece, tile), piece)
            added = part[here, :].astype(jnp.float32) + source[there, :].astype(jnp.float32)
            part[here, :] = added.astype(jnp.bfloat16)
            return carry

        lax.fori_loop(0, rows // piece, body, 0)

    def remote(src, dst, send_sem, recv_sem, device):
        return pltpu.make_async_remote_copy(
            src_ref=src,
            dst_ref=dst,
            send_sem=send_sem,
            recv_sem=recv_sem,
            device_id=device,
            device_id_type=MESH,
        )

    def rows_at(ref, at, rows):
        return ref.at[pl.ds(pl.multiple_of(at, tile), rows)]

    def mine_at(h, step):
        return lax.rem(lax.div(q, 1 << (step if h == 0 else steps - 1 - step)), 2)

    def pieces(h, step, size):
        if step >= steps:
            return [(0, size)]
        mine = mine_at(h, step)
        return [((1 - mine) * (size // 2), size // 2), (mine * (size // 2), size // 2)]

    def tile_sum(part, at, source, source_at, t):
        here = pl.ds(pl.multiple_of(at + t * tile, tile), tile)
        there = pl.ds(pl.multiple_of(source_at + t * tile, tile), tile)
        return part[here, :].astype(jnp.float32) + source[there, :].astype(jnp.float32)

    def finish(part, phase, h, at, source, source_at):
        if phase == chunks - 1:
            for t in range(half_tiles // 2):
                even, odd = (
                    jnp.maximum(tile_sum(part, at, source, source_at, 2 * t + i), 0.0) for i in range(2)
                )
                for made, value in (
                    (first, jnp.where(low, even, turned(odd))),
                    (second, jnp.where(low, turned(even), odd)),
                ):
                    own(made, h * (half_tiles // 2) + t, 1)[...] = value.astype(jnp.bfloat16)[None]
        elif phase < chunks:
            for t in range(half_tiles):
                hidden = jnp.maximum(tile_sum(part, at, source, source_at, t), 0.0).astype(jnp.bfloat16)
                own(phase + chunks, h * half_tiles + t, 1)[...] = hidden[None]
        elif phase < first:
            lanes = (phase - chunks) * LANES
            for t in range(half_tiles):
                rows = (h * half_tiles + t) * tile
                added = tile_sum(part, at, source, source_at, t)
                out[rows : rows + tile, lanes : lanes + LANES] = added.astype(jnp.bfloat16)
        else:
            lanes = (chunks - 1) * LANES
            for t in range(half_tiles // 2):
                rows = (h * (half_tiles // 2) + t) * tile
                added = tile_sum(part, at, source, source_at, t)
                if phase == first:
                    held[rows : rows + tile, :] = added.astype(jnp.bfloat16)
                else:
                    before = held[rows : rows + tile, :].astype(jnp.float32)
                    even = jnp.where(low, before, turned(added)).astype(jnp.bfloat16)
                    odd = jnp.where(low, turned(before), added).astype(jnp.bfloat16)
                    out[2 * rows : 2 * rows + tile, lanes : lanes + LANES] = even
                    out[2 * rows + tile : 2 * (rows + tile), lanes : lanes + LANES] = odd

    def reduce(phase, started):
        narrow = phase >= first
        part = thin_part if narrow else wide_part
        block = node_tiles(phase) // 2 * tile
        half_rows = n_q * block
        region = 4 * half_rows if phase == second else 0
        cuts = [pieces(h, 0, half_rows) for h in range(2)]
        arrived = [[], []]
        for k in range(len(cuts[0])):
            for h in range(2):
                off, rows = cuts[h][k]
                place_rows(part, region // tile, 1 - b0, h, lax.div(off, block), rows // block, narrow)
                copy = remote(
                    rows_at(part, region + ((1 - b0) * 2 + h) * half_rows + off, rows),
                    rows_at(core_in[phase], h * half_rows + off, rows),
                    c_send.at[phase % SETS, h, k],
                    c_recv.at[phase % SETS, h, k],
                    partners[0],
                )
                copy.start()
                started.append(copy)
                arrived[h].append((copy, core_in[phase], h * half_rows + off, off, rows))
        for k in range(len(cuts[0])):
            for h in range(2):
                off, rows = cuts[h][k]
                place_rows(part, region // tile, b0, h, lax.div(off, block), rows // block, narrow)
        base = [region + (b0 * 2 + h) * half_rows for h in range(2)]
        yield

        def take(h, k):
            copy, source, source_at, off, rows = arrived[h][k]
            copy.wait_recv()
            add_in(part, base[h] + off, source, source_at, rows)

        size = half_rows
        for step in range(steps):
            following = [[], []]
            for h in range(2):
                take(h, 0)
                bit = step if h == 0 else steps - 1 - step
                away = base[h] + (1 - mine_at(h, step)) * (size // 2)
                landing = (h * (n_q - 1) + n_q - (n_q >> step)) * block
                for k, (off, rows) in enumerate(pieces(h, step + 1, size // 2)):
                    copy = remote(
                        rows_at(part, away + off, rows),
                        rows_at(step_in[phase], landing + off, rows),
                        s_send.at[phase % SETS, h, step, k],
                        s_recv.at[phase % SETS, h, step, k],
                        partners[1 + bit],
                    )
                    copy.start()
                    started.append(copy)
                    following[h].append((copy, step_in[phase], landing + off, off, rows))
            if step == steps - 1:
                yield
            for h in range(2):
                take(h, 1)
                base[h] = base[h] + mine_at(h, step) * (size // 2)
            size //= 2
            arrived = following
            if step == 0 and phase < first - 1:
                relay_near(phase + 1)
                if phase + 1 < chunks:
                    relay_far(phase + 1)
            if step == 0:
                yield
        for h in range(2):
            copy, source, source_at, off, rows = arrived[h][0]
            copy.wait_recv()
            finish(part, phase, h, base[h], source, source_at)

    w1_load.wait()
    for k in range(PARTS):
        feat_loads[k].wait()
        project(0, k)
        if k == 0:
            pl.semaphore_wait(barrier, greeted)
        start_all(inner_sends(0, k, (1,)))
        start_all(outer_sends(0, k))
    for k in range(PARTS):
        start_all(inner_sends(0, k, range(2, n_row)))
    for chunk in range(1, chunks):
        for k in range(PARTS):
            project(chunk, k)
    pl.when(outer(r))(lambda: own_inner(1))
    vals[slots] = jnp.zeros((tile, tile), vals.dtype)
    sums[pairs_total] = jnp.zeros((tile, LANES), sums.dtype)
    slot_at, col_at, keep_at, last = pair_plan(
        row_ids[...], col_ids[...], filled[0, 0], n_col * per_dev, pairs_total, plan.shape[1]
    )
    plan_v[0:1, :] = slot_at
    plan_v[1:2, :] = col_at
    plan_v[2:3, : last.shape[1]] = last
    keep_v[0:1, :] = keep_at
    moves = [
        pltpu.make_async_copy(plan_v, plan, plan_sem.at[0]),
        pltpu.make_async_copy(keep_v, keep, plan_sem.at[1]),
    ]
    for move in moves:
        move.start()
    relay_all(0)
    for move in moves:
        move.wait()
    for load in loads:
        load.wait()
    pl.when(inner(r))(lambda: own_inner(1))
    own_outer(1)
    started = []
    for phase in range(first):
        gathered(phase)
        if phase == first - 1:
            relay_near(first)
            own_outer(second)
        compute(panels[phase])
        work = reduce(phase, started)
        if phase == first - 1:
            break
        for _ in work:
            pass
        made = []
        if phase < chunks:
            made = [first, second] if phase == chunks - 1 else [phase + chunks]
        for later in made:
            if later >= SETS:
                drain(later - SETS)
            own_inner(later)
        if phase + 1 >= chunks:
            relay_far(phase + 1)
        for later in made[:1]:
            own_outer(later)
        for copy in started:
            copy.wait_send()
        started.clear()
    next(work)
    next(work)
    relay_far(first)
    relay_near(second)
    next(work)
    gathered_spread(first)
    compute(spread)
    relay_far(second)
    work_first = reduce(first, started)
    next(work_first)
    next(work_first)
    for _ in work:
        pass
    gathered_spread(second)
    total = compute(spread, 0, UNROLL_PARTS // 2)
    next(work_first)
    compute(spread, UNROLL_PARTS // 2, UNROLL_PARTS, total)
    work_second = reduce(second, started)
    next(work_second)
    next(work_second)
    for rest in (work_first, work_second):
        for _ in rest:
            pass
    for copy in started:
        copy.wait_send()
    for phase in range(phases - SETS, phases):
        drain(phase)


def shards(n_row, n_col, features, tile_values, tile_rows, tile_cols, tile_count, w_first, w_second):
    slots, tile = tile_values.shape[2], tile_values.shape[-1]
    node_dev, width = features.shape
    row_tiles = node_dev * n_col // tile
    chunks = width // LANES
    phases = 2 * chunks + 1
    shares = [1] * (phases - 2) + [2, 2]
    pairs_total = -(-(slots + row_tiles) // (2 * UNROLL_PARTS)) * UNROLL_PARTS
    n_q = n_col // 2
    steps = n_q.bit_length() - 1
    plan_width = -(-2 * pairs_total // LANES) * LANES
    half = node_dev // 2
    vmem = pl.BlockSpec(memory_space=pltpu.VMEM)
    smem = pl.BlockSpec(memory_space=pltpu.SMEM)
    bf16 = jnp.bfloat16
    dma = pltpu.SemaphoreType.DMA
    aggregate = pl.pallas_call(
        functools.partial(kernel, n_row, n_col, chunks, pairs_total),
        name="gcn",
        out_shape=pltpu.VMEM((node_dev, width), bf16),
        in_specs=[smem] + [vmem] * 2 + [pl.BlockSpec(memory_space=pltpu.HBM)] * 3,
        out_specs=vmem,
        scratch_shapes=[pltpu.VMEM((n_row * node_dev // tile // share, tile, LANES), bf16) for share in shares]
        + [pltpu.VMEM((2 * n_q * half // share, LANES), bf16) for share in shares]
        + [pltpu.VMEM((2 * (n_q - 1) * half // share, LANES), bf16) for share in shares]
        + [
            pltpu.VMEM((node_dev, width), bf16),
            pltpu.VMEM((width, width), bf16),
            pltpu.VMEM((slots + 1, tile, tile), bf16),
            pltpu.VMEM((pairs_total + 1, tile, LANES), bf16),
            pltpu.VMEM((n_col * node_dev, LANES), bf16),
            pltpu.VMEM((n_col * node_dev, LANES), bf16),
            pltpu.VMEM((n_row * node_dev // tile, tile, LANES), bf16),
            pltpu.VMEM((node_dev // 2, LANES), bf16),
            pltpu.VMEM((8, plan_width), jnp.int32),
            pltpu.VMEM((8, plan_width), jnp.float32),
            pltpu.SMEM((8, plan_width), jnp.int32),
            pltpu.SMEM((8, plan_width), jnp.float32),
            dma((2,)),
            dma((1 + PARTS,)),
            dma((LOADS,)),
            dma((SETS, 2 * n_row - 2, PARTS)),
            dma((phases, 2 * n_row - 2, PARTS)),
            dma((SETS, 2, 2)),
            dma((SETS, 2, 2)),
            dma((SETS, 2, steps, 2)),
            dma((SETS, 2, steps, 2)),
        ],
        compiler_params=pltpu.CompilerParams(
            collective_id=0, has_side_effects=True, vmem_limit_bytes=63 * 1024 * 1024
        ),
    )(tile_count, tile_rows[0], tile_cols[0], features, w_first, tile_values[0, 0])
    product = jnp.dot(aggregate, w_second, preferred_element_type=jnp.float32)
    return jax.nn.relu(product).astype(bf16)


def solution(mesh):
    return jax.shard_map(
        functools.partial(shards, mesh.shape["row"], mesh.shape["col"]),
        mesh=mesh,
        in_specs=(
            P(("row", "col"), None),
            P("row", "col", None, None, None),
            P("row", "col", None),
            P("row", "col", None),
            P("row", "col"),
            P(),
            P(),
        ),
        out_specs=P(("row", "col"), None),
        check_vma=False,
    )
```

```python
import functools

import jax
import jax.numpy as jnp
from jax import lax
from jax.experimental import pallas as pl
from jax.experimental.pallas import tpu as pltpu
from jax.sharding import PartitionSpec as P

LANES = 128
UNROLL_PARTS = 2
LOADS = 4
SETS = 3
PARTS = 2
ROWS_AT_ONCE = 256
MESH = pl.DeviceIdType.MESH


def iota(shape, axis):
    return lax.broadcasted_iota(jnp.int32, shape, axis)


def pair_plan(row_ids, col_ids, filled, row_tiles, pairs_total, width):
    slots = row_ids.shape[1]
    one, zero = jnp.int32(1), jnp.int32(0)

    def down(mask):
        return jnp.sum(mask, axis=0, keepdims=True)

    def across(mask):
        return jnp.sum(mask, axis=1, keepdims=True)

    square = (slots, slots)
    lane, sub = iota(square, 1), iota(square, 0)
    rows_l = jnp.where(iota((1, slots), 1) < filled, row_ids, -1)
    rows_s = across(jnp.where(lane == sub, rows_l, zero))
    cols_s = across(jnp.where(lane == sub, col_ids, zero))
    rank_s = across(jnp.where((rows_s == rows_l) & (lane < sub), one, zero))
    hit = jnp.where(rows_s == iota((slots, row_tiles), 1), one, zero)
    hit_t = jnp.where(rows_l == iota((row_tiles, slots), 0), one, zero)
    count_l, count_s = down(hit), across(hit_t)
    pairs_l, pairs_s = (count_l + 1) >> 1, (count_s + 1) >> 1
    box = (row_tiles, row_tiles)
    start_l = down(jnp.where(iota(box, 0) < iota(box, 1), pairs_s, zero))
    start_s = across(jnp.where(iota(box, 1) < iota(box, 0), pairs_l, zero))
    place_s = jnp.where(rows_s >= 0, 2 * across(hit * start_l) + rank_s, -one)
    here = place_s == iota((slots, width), 1)
    slot_ids = iota((slots, width), 0)
    slot_at = slots + down(jnp.where(here, slot_ids - slots, zero))
    col_at = down(jnp.where(here, cols_s, zero))
    opens = (start_s == iota((row_tiles, width), 1)) & (count_s > 0)
    keep = one - down(jnp.where(opens, one, zero))
    last = jnp.where(count_l > 0, start_l + pairs_l - 1, jnp.int32(pairs_total))
    return slot_at, col_at, keep.astype(jnp.float32), last


def kernel(n_row, n_col, chunks, pairs_total, filled_hbm, rows_hbm, cols_hbm, feat_hbm, w1_hbm, vals_hbm, out, *scratch):
    phases = 2 * chunks + 1
    first, second = phases - 2, phases - 1
    panels = scratch[:phases]
    core_in = scratch[phases : 2 * phases]
    step_in = scratch[2 * phases : 3 * phases]
    feat, w1, vals, sums, wide_part, thin_part, spread, held = scratch[3 * phases : 3 * phases + 8]
    filled, row_ids, col_ids, plan_v, keep_v, plan, keep, plan_sem = scratch[3 * phases + 8 : 3 * phases + 16]
    in_sem, load_sem, g_send, g_recv, c_send, c_recv, s_send, s_recv = scratch[3 * phases + 16 :]
    slots, tile, _ = vals_hbm.shape
    node_dev, width = feat.shape
    per_dev = node_dev // tile
    half_tiles = per_dev // 2
    n_q = n_col // 2
    steps = n_q.bit_length() - 1
    low = iota((tile, LANES), 1) < LANES // 2
    r, c = lax.axis_index("row"), lax.axis_index("col")
    b0 = lax.rem(c, 2)
    q = lax.div(c, 2)

    cut = per_dev // PARTS
    cut_rows = cut * tile
    feat_loads = [
        pltpu.make_async_copy(
            feat_hbm.at[pl.ds(k * cut_rows, cut_rows)], feat.at[pl.ds(k * cut_rows, cut_rows)], in_sem.at[k + 1]
        )
        for k in range(PARTS)
    ]
    w1_load = pltpu.make_async_copy(w1_hbm, w1, in_sem.at[0])
    w1_load.start()
    for load in feat_loads:
        load.start()
    id_loads = [
        pltpu.make_async_copy(source, target, in_sem.at[1 + PARTS + i])
        for i, (source, target) in enumerate(
            [(filled_hbm, filled), (rows_hbm, row_ids), (cols_hbm, col_ids)]
        )
    ]
    for load in id_loads:
        load.start()

    barrier = pltpu.get_barrier_semaphore()
    partners = []
    for bit in range(steps + 1):
        mine = lax.rem(lax.div(c, 1 << bit), 2)
        partners.append((r, c + (1 - 2 * mine) * (1 << bit)))
    for device in partners:
        pl.semaphore_signal(barrier, inc=1, device_id=device, device_id_type=MESH)
    greeted = jnp.int32(len(partners))
    last_row = n_row - 1
    distances = [d * sign for d in range(last_row, 0, -1) for sign in (1, -1)]

    def inner(node):
        return (node > 0) & (node < last_row)

    def outer(node):
        return (node == 0) | (node == last_row)

    for d in distances:
        there = r + d
        valid = (there >= 0) & (there <= last_row)
        reached = valid if abs(d) == 1 else valid & inner(there)
        greeted = greeted + reached.astype(jnp.int32)

        @pl.when(valid if abs(d) == 1 else valid & inner(r))
        def _(there=there):
            pl.semaphore_signal(barrier, inc=1, device_id=(there, c), device_id_type=MESH)

    share = slots // LOADS
    loads = [
        pltpu.make_async_copy(
            vals_hbm.at[pl.ds(i * share, share)], vals.at[pl.ds(i * share, share)], load_sem.at[i]
        )
        for i in range(LOADS)
    ]
    for load in loads:
        load.start()

    def node_tiles(phase):
        return per_dev // 2 if phase >= first else per_dev

    def own(phase, offset, rows):
        return panels[phase].at[pl.ds(r * node_tiles(phase) + offset, rows)]

    def turned(value):
        return pltpu.roll(value, LANES // 2, 1)

    def project(chunk, k):
        size = min(cut_rows, ROWS_AT_ONCE)
        for at in range(k * cut_rows, (k + 1) * cut_rows, size):
            product = jnp.dot(
                feat[at : at + size, :],
                w1[:, chunk * LANES : (chunk + 1) * LANES],
                preferred_element_type=jnp.float32,
            )
            tiles = size // tile
            own(chunk, at // tile, tiles)[...] = product.astype(jnp.bfloat16).reshape(tiles, tile, LANES)

    def way(d):
        return d - 1 if d > 0 else last_row - 1 - d

    def node_copy(phase, origin, d, k, device):
        share = node_tiles(phase) // PARTS
        view = panels[phase].at[pl.ds(origin * node_tiles(phase) + k * share, share)]
        return pltpu.make_async_remote_copy(
            src_ref=view,
            dst_ref=view,
            send_sem=g_send.at[phase % SETS, way(d), k],
            recv_sem=g_recv.at[phase, origin if d > 0 else origin - 1, k],
            device_id=(device, c),
            device_id_type=MESH,
        )

    def inner_sends(phase, k, reaches=range(1, n_row)):
        for d in distances:
            if abs(d) not in reaches:
                continue
            target = r + d
            yield inner(target), node_copy(phase, r, d, k, target)

    def outer_sends(phase, k):
        for d in (1, -1):
            target = r + d
            yield outer(target), node_copy(phase, r, d, k, target)

    def relays(phase, near, k):
        for sign in (1, -1):
            origin = r - sign * near
            place = n_row - 2 if sign > 0 else 1
            valid = (r == place) & (origin >= 0) & (origin <= last_row)
            arrived = node_copy(phase, origin, sign * near, k, r)
            forward = node_copy(phase, origin, sign * (near + 1), k, r + sign)
            yield valid, arrived, forward

    def start_all(sends):
        for valid, copy in sends:
            pl.when(valid)(copy.start)

    def own_inner(phase):
        for reach in range(last_row, 0, -1):
            for k in range(PARTS):
                start_all(inner_sends(phase, k, (reach,)))

    def own_outer(phase):
        if phase < phases:
            for k in range(PARTS):
                start_all(outer_sends(phase, k))

    def relay(phase, near, k):
        if phase < phases:
            for valid, arrived, forward in relays(phase, near, k):

                @pl.when(valid)
                def _(arrived=arrived, forward=forward):
                    arrived.wait_recv()
                    forward.start()

    def relay_far(phase):
        for near in range(2, last_row):
            for k in range(PARTS):
                relay(phase, near, k)

    def relay_near(phase):
        for k in range(PARTS):
            relay(phase, 1, k)

    def relay_all(phase):
        relay_near(phase)
        relay_far(phase)

    def arrive(phase, d, k):
        origin = r - d
        relayed = r == (n_row - 2 if d > 0 else 1)
        valid = (origin >= 0) & (origin <= last_row) & jnp.logical_not(relayed)
        pl.when(valid)(node_copy(phase, origin, d, k, r).wait_recv)

    def gathered(phase):
        for k in range(PARTS):
            for d in sorted(distances, key=abs):
                arrive(phase, d, k)

    def spread_node(phase, origin):
        def body(i, carry):
            at = origin * (per_dev // 2) + i
            pair = panels[phase][at].astype(jnp.float32)
            other = turned(pair)
            spread[2 * at] = jnp.where(low, pair, other).astype(jnp.bfloat16)
            spread[2 * at + 1] = jnp.where(low, other, pair).astype(jnp.bfloat16)
            return carry

        lax.fori_loop(0, per_dev // 2, body, 0, unroll=True)

    def gathered_spread(phase):
        spread_node(phase, r)
        for d in sorted(distances, key=abs):
            for k in range(PARTS):
                arrive(phase, d, k)

            @pl.when((r - d >= 0) & (r - d <= last_row))
            def _(d=d):
                spread_node(phase, r - d)

    def drain(phase):
        for k in range(PARTS):
            for valid, copy in [*inner_sends(phase, k), *outer_sends(phase, k)]:
                pl.when(valid)(copy.wait_send)
            for near in range(1, last_row):
                for valid, _, forward in relays(phase, near, k):
                    pl.when(valid)(forward.wait_send)

    unroll = pairs_total // UNROLL_PARTS

    def compute(panel, low_trip=0, high_trip=UNROLL_PARTS, total=None):
        def one(p, acc):
            left = [vals[plan[0, 2 * p + k]] for k in range(2)]
            right = [panel[plan[1, 2 * p + k]] for k in range(2)]
            product = jnp.dot(
                jnp.concatenate(left, axis=1),
                jnp.concatenate(right, axis=0),
                preferred_element_type=jnp.float32,
            )
            acc = acc * keep[0, p] + product
            sums[p] = acc.astype(jnp.bfloat16)
            return acc

        def body(i, acc):
            for u in range(unroll):
                acc = one(i * unroll + u, acc)
            return acc

        if total is None:
            total = jnp.zeros((tile, LANES), jnp.float32)
        return lax.fori_loop(low_trip, high_trip, body, total)

    def place_rows(part, region, parity, h, at, count, narrow):
        taken = half_tiles // 2 if narrow else half_tiles

        def body(i, carry):
            rev = sum(lax.rem(lax.div(at + i, 1 << k), 2) * (1 << (steps - 1 - k)) for k in range(steps))
            dest = 2 * (rev if h == 0 else at + i) + parity
            base = region + ((parity * 2 + h) * n_q + at + i) * taken
            row_tile = dest * per_dev + h * half_tiles
            for t in range(taken):
                if narrow:
                    rows = jnp.where(
                        low, sums[plan[2, row_tile + 2 * t]], sums[plan[2, row_tile + 2 * t + 1]]
                    )
                else:
                    rows = sums[plan[2, row_tile + t]]
                part[pl.ds(pl.multiple_of((base + t) * tile, tile), tile), :] = rows
            return carry

        lax.fori_loop(0, count, body, 0)

    def add_in(part, at, source, source_at, rows):
        piece = min(rows, ROWS_AT_ONCE)

        def body(i, carry):
            here = pl.ds(pl.multiple_of(at + i * piece, tile), piece)
            there = pl.ds(pl.multiple_of(source_at + i * piece, tile), piece)
            added = part[here, :].astype(jnp.float32) + source[there, :].astype(jnp.float32)
            part[here, :] = added.astype(jnp.bfloat16)
            return carry

        lax.fori_loop(0, rows // piece, body, 0)

    def remote(src, dst, send_sem, recv_sem, device):
        return pltpu.make_async_remote_copy(
            src_ref=src,
            dst_ref=dst,
            send_sem=send_sem,
            recv_sem=recv_sem,
            device_id=device,
            device_id_type=MESH,
        )

    def rows_at(ref, at, rows):
        return ref.at[pl.ds(pl.multiple_of(at, tile), rows)]

    def mine_at(h, step):
        return lax.rem(lax.div(q, 1 << (step if h == 0 else steps - 1 - step)), 2)

    def pieces(h, step, size):
        if step >= steps:
            return [(0, size)]
        mine = mine_at(h, step)
        return [((1 - mine) * (size // 2), size // 2), (mine * (size // 2), size // 2)]

    def tile_sum(part, at, source, source_at, t):
        here = pl.ds(pl.multiple_of(at + t * tile, tile), tile)
        there = pl.ds(pl.multiple_of(source_at + t * tile, tile), tile)
        return part[here, :].astype(jnp.float32) + source[there, :].astype(jnp.float32)

    def finish(part, phase, h, at, source, source_at):
        if phase == chunks - 1:
            for t in range(half_tiles // 2):
                even, odd = (
                    jnp.maximum(tile_sum(part, at, source, source_at, 2 * t + i), 0.0) for i in range(2)
                )
                for made, value in (
                    (first, jnp.where(low, even, turned(odd))),
                    (second, jnp.where(low, turned(even), odd)),
                ):
                    own(made, h * (half_tiles // 2) + t, 1)[...] = value.astype(jnp.bfloat16)[None]
        elif phase < chunks:
            for t in range(half_tiles):
                hidden = jnp.maximum(tile_sum(part, at, source, source_at, t), 0.0).astype(jnp.bfloat16)
                own(phase + chunks, h * half_tiles + t, 1)[...] = hidden[None]
        elif phase < first:
            lanes = (phase - chunks) * LANES
            for t in range(half_tiles):
                rows = (h * half_tiles + t) * tile
                added = tile_sum(part, at, source, source_at, t)
                out[rows : rows + tile, lanes : lanes + LANES] = added.astype(jnp.bfloat16)
        else:
            lanes = (chunks - 1) * LANES
            for t in range(half_tiles // 2):
                rows = (h * (half_tiles // 2) + t) * tile
                added = tile_sum(part, at, source, source_at, t)
                if phase == first:
                    held[rows : rows + tile, :] = added.astype(jnp.bfloat16)
                else:
                    before = held[rows : rows + tile, :].astype(jnp.float32)
                    even = jnp.where(low, before, turned(added)).astype(jnp.bfloat16)
                    odd = jnp.where(low, turned(before), added).astype(jnp.bfloat16)
                    out[2 * rows : 2 * rows + tile, lanes : lanes + LANES] = even
                    out[2 * rows + tile : 2 * (rows + tile), lanes : lanes + LANES] = odd

    def reduce(phase, started):
        narrow = phase >= first
        part = thin_part if narrow else wide_part
        block = node_tiles(phase) // 2 * tile
        half_rows = n_q * block
        region = 4 * half_rows if phase == second else 0
        cuts = [pieces(h, 0, half_rows) for h in range(2)]
        arrived = [[], []]
        for k in range(len(cuts[0])):
            for h in range(2):
                off, rows = cuts[h][k]
                place_rows(part, region // tile, 1 - b0, h, lax.div(off, block), rows // block, narrow)
                copy = remote(
                    rows_at(part, region + ((1 - b0) * 2 + h) * half_rows + off, rows),
                    rows_at(core_in[phase], h * half_rows + off, rows),
                    c_send.at[phase % SETS, h, k],
                    c_recv.at[phase % SETS, h, k],
                    partners[0],
                )
                copy.start()
                started.append(copy)
                arrived[h].append((copy, core_in[phase], h * half_rows + off, off, rows))
        for k in range(len(cuts[0])):
            for h in range(2):
                off, rows = cuts[h][k]
                place_rows(part, region // tile, b0, h, lax.div(off, block), rows // block, narrow)
        base = [region + (b0 * 2 + h) * half_rows for h in range(2)]
        yield

        def take(h, k):
            copy, source, source_at, off, rows = arrived[h][k]
            copy.wait_recv()
            add_in(part, base[h] + off, source, source_at, rows)

        size = half_rows
        for step in range(steps):
            following = [[], []]
            for h in range(2):
                take(h, 0)
                bit = step if h == 0 else steps - 1 - step
                away = base[h] + (1 - mine_at(h, step)) * (size // 2)
                landing = (h * (n_q - 1) + n_q - (n_q >> step)) * block
                for k, (off, rows) in enumerate(pieces(h, step + 1, size // 2)):
                    copy = remote(
                        rows_at(part, away + off, rows),
                        rows_at(step_in[phase], landing + off, rows),
                        s_send.at[phase % SETS, h, step, k],
                        s_recv.at[phase % SETS, h, step, k],
                        partners[1 + bit],
                    )
                    copy.start()
                    started.append(copy)
                    following[h].append((copy, step_in[phase], landing + off, off, rows))
            if step == steps - 1:
                yield
            for h in range(2):
                take(h, 1)
                base[h] = base[h] + mine_at(h, step) * (size // 2)
            size //= 2
            arrived = following
            if step == 0 and phase < first - 1:
                relay_near(phase + 1)
                if phase + 1 < chunks:
                    relay_far(phase + 1)
            if step == 0:
                yield
        for h in range(2):
            copy, source, source_at, off, rows = arrived[h][0]
            copy.wait_recv()
            finish(part, phase, h, base[h], source, source_at)

    w1_load.wait()
    for k in range(PARTS):
        feat_loads[k].wait()
        project(0, k)
        if k == 0:
            pl.semaphore_wait(barrier, greeted)
        start_all(inner_sends(0, k, (1,)))
        start_all(outer_sends(0, k))
    for k in range(PARTS):
        start_all(inner_sends(0, k, range(2, n_row)))
    for chunk in range(1, chunks):
        for k in range(PARTS):
            project(chunk, k)
    pl.when(outer(r))(lambda: own_inner(1))
    vals[slots] = jnp.zeros((tile, tile), vals.dtype)
    sums[pairs_total] = jnp.zeros((tile, LANES), sums.dtype)
    for load in id_loads:
        load.wait()
    slot_at, col_at, keep_at, last = pair_plan(
        row_ids[...], col_ids[...], filled[...], n_col * per_dev, pairs_total, plan.shape[1]
    )
    plan_v[0:1, :] = slot_at
    plan_v[1:2, :] = col_at
    plan_v[2:3, : last.shape[1]] = last
    keep_v[0:1, :] = keep_at
    moves = [
        pltpu.make_async_copy(plan_v, plan, plan_sem.at[0]),
        pltpu.make_async_copy(keep_v, keep, plan_sem.at[1]),
    ]
    for move in moves:
        move.start()
    relay_all(0)
    for move in moves:
        move.wait()
    for load in loads:
        load.wait()
    pl.when(inner(r))(lambda: own_inner(1))
    own_outer(1)
    started = []
    for phase in range(first):
        gathered(phase)
        if phase == first - 1:
            relay_near(first)
        compute(panels[phase])
        work = reduce(phase, started)
        if phase == first - 1:
            break
        for _ in work:
            pass
        made = []
        if phase < chunks:
            made = [first, second] if phase == chunks - 1 else [phase + chunks]
        for later in made:
            if later >= SETS:
                drain(later - SETS)
            own_inner(later)
        if phase + 1 >= chunks:
            relay_far(phase + 1)
        for later in made[:1]:
            own_outer(later)
        for copy in started:
            copy.wait_send()
        started.clear()
    next(work)
    next(work)
    relay_far(first)
    own_outer(second)
    relay_near(second)
    next(work)
    gathered_spread(first)
    compute(spread)
    relay_far(second)
    work_first = reduce(first, started)
    next(work_first)
    next(work_first)
    for _ in work:
        pass
    gathered_spread(second)
    total = compute(spread, 0, UNROLL_PARTS // 2)
    next(work_first)
    compute(spread, UNROLL_PARTS // 2, UNROLL_PARTS, total)
    work_second = reduce(second, started)
    next(work_second)
    next(work_second)
    for rest in (work_first, work_second):
        for _ in rest:
            pass
    for copy in started:
        copy.wait_send()
    for phase in range(phases - SETS, phases):
        drain(phase)


def shards(n_row, n_col, features, tile_values, tile_rows, tile_cols, tile_count, w_first, w_second):
    slots, tile = tile_values.shape[2], tile_values.shape[-1]
    node_dev, width = features.shape
    row_tiles = node_dev * n_col // tile
    chunks = width // LANES
    phases = 2 * chunks + 1
    shares = [1] * (phases - 2) + [2, 2]
    pairs_total = -(-(slots + row_tiles) // (2 * UNROLL_PARTS)) * UNROLL_PARTS
    n_q = n_col // 2
    steps = n_q.bit_length() - 1
    plan_width = -(-2 * pairs_total // LANES) * LANES
    half = node_dev // 2
    vmem = pl.BlockSpec(memory_space=pltpu.VMEM)
    bf16 = jnp.bfloat16
    dma = pltpu.SemaphoreType.DMA
    aggregate = pl.pallas_call(
        functools.partial(kernel, n_row, n_col, chunks, pairs_total),
        name="gcn",
        out_shape=pltpu.VMEM((node_dev, width), bf16),
        in_specs=[pl.BlockSpec(memory_space=pltpu.HBM)] * 6,
        out_specs=vmem,
        scratch_shapes=[pltpu.VMEM((n_row * node_dev // tile // share, tile, LANES), bf16) for share in shares]
        + [pltpu.VMEM((2 * n_q * half // share, LANES), bf16) for share in shares]
        + [pltpu.VMEM((2 * (n_q - 1) * half // share, LANES), bf16) for share in shares]
        + [
            pltpu.VMEM((node_dev, width), bf16),
            pltpu.VMEM((width, width), bf16),
            pltpu.VMEM((slots + 1, tile, tile), bf16),
            pltpu.VMEM((pairs_total + 1, tile, LANES), bf16),
            pltpu.VMEM((n_col * node_dev, LANES), bf16),
            pltpu.VMEM((n_col * node_dev, LANES), bf16),
            pltpu.VMEM((n_row * node_dev // tile, tile, LANES), bf16),
            pltpu.VMEM((node_dev // 2, LANES), bf16),
            pltpu.VMEM((1, 1), jnp.int32),
            pltpu.VMEM((1, slots), jnp.int32),
            pltpu.VMEM((1, slots), jnp.int32),
            pltpu.VMEM((8, plan_width), jnp.int32),
            pltpu.VMEM((8, plan_width), jnp.float32),
            pltpu.SMEM((8, plan_width), jnp.int32),
            pltpu.SMEM((8, plan_width), jnp.float32),
            dma((2,)),
            dma((4 + PARTS,)),
            dma((LOADS,)),
            dma((SETS, 2 * n_row - 2, PARTS)),
            dma((phases, n_row - 1, PARTS)),
            dma((SETS, 2, 2)),
            dma((SETS, 2, 2)),
            dma((SETS, 2, steps, 2)),
            dma((SETS, 2, steps, 2)),
        ],
        compiler_params=pltpu.CompilerParams(
            collective_id=0, has_side_effects=True, vmem_limit_bytes=63 * 1024 * 1024
        ),
    )(tile_count, tile_rows[0], tile_cols[0], features, w_first, tile_values[0, 0])
    product = jnp.dot(aggregate, w_second, preferred_element_type=jnp.float32)
    return jax.nn.relu(product).astype(bf16)


def solution(mesh):
    return jax.shard_map(
        functools.partial(shards, mesh.shape["row"], mesh.shape["col"]),
        mesh=mesh,
        in_specs=(
            P(("row", "col"), None),
            P("row", "col", None, None, None),
            P("row", "col", None),
            P("row", "col", None),
            P("row", "col"),
            P(),
            P(),
        ),
        out_specs=P(("row", "col"), None),
        check_vma=False,
    )
```
